32 devices in a mesh: data: 1 (over z), outer: 4 (over y), dap: 8 (over x, core).
Axes of the slice: x: 4, y: 4, z: 1, core: 2. Of those that a mesh axis runs over, the one named last changes fastest.
The devices are a block of a 4x4x8 slice.
Arguments:
- msa_rep: bfloat16 [256, 128, 256], P('data', ('outer', 'dap'))
- msa_mask: int32 [256, 128], P('data')
- pair_rep: float32 [128, 128, 128], P(('data', 'outer', 'dap'))
- ln_gamma: bfloat16 [256], replicated
- ln_beta: bfloat16 [256], replicated
- w_left: bfloat16 [256, 32], replicated
- b_left: bfloat16 [32], replicated
- w_right: bfloat16 [256, 32], replicated
- b_right: bfloat16 [32], replicated
- w_out: bfloat16 [1024, 128], replicated
- b_out: bfloat16 [128], replicated
Outputs:
- output 1: float32 [128, 128, 128], P(('data', 'outer', 'dap'))
- output 2: bfloat16 [256, 128, 256], P(('data', 'outer', 'dap'))
All inputs are finite; a program needn't handle non-finite values.
Results may differ from the reference program's by a relative error of at most 0.00395037.
Values are sent between devices in bfloat16 or wider.
A program may use at most 768 MiB of HBM per device.

```python
import math
import jax
import jax.numpy as jnp
from jax import lax

NUM_SEQ = 256
NUM_RES = 128
MSA_DIM = 256
PAIR_DIM = 128
OPM_DIM = 32


def setup_inputs(seed: int = 0, part: int = 0) -> dict:
    part_keys = jax.random.split(jax.random.fold_in(jax.random.key(seed), part), 5)
    shared_keys = jax.random.split(jax.random.key(seed + 1), 8)
    profile = jax.random.normal(part_keys[0], (1, NUM_RES, MSA_DIM), jnp.float32)
    noise_msa = jax.random.normal(part_keys[1], (NUM_SEQ, NUM_RES, MSA_DIM), jnp.float32)
    msa_rep = (profile + 0.7 * noise_msa).astype(jnp.bfloat16)
    coverage = jax.random.randint(part_keys[2], (NUM_SEQ, 1), 35, 100)
    mask_draws = jax.random.randint(part_keys[3], (NUM_SEQ, NUM_RES), 0, 100)
    msa_mask = (mask_draws < coverage).astype(jnp.int32)
    pair_rep = jax.random.normal(part_keys[4], (NUM_RES, NUM_RES, PAIR_DIM), jnp.float32)
    ln_gamma = (1.0 + 0.3 * jax.random.normal(shared_keys[0], (MSA_DIM,), jnp.float32)).astype(jnp.bfloat16)
    ln_beta = (0.5 * jax.random.normal(shared_keys[1], (MSA_DIM,), jnp.float32)).astype(jnp.bfloat16)
    w_left = (jax.random.normal(shared_keys[2], (MSA_DIM, OPM_DIM), jnp.float32) * MSA_DIM ** -0.5).astype(jnp.bfloat16)
    b_left = (0.5 * jax.random.normal(shared_keys[3], (OPM_DIM,), jnp.float32)).astype(jnp.bfloat16)
    w_right = (jax.random.normal(shared_keys[4], (MSA_DIM, OPM_DIM), jnp.float32) * MSA_DIM ** -0.5).astype(jnp.bfloat16)
    b_right = (0.5 * jax.random.normal(shared_keys[5], (OPM_DIM,), jnp.float32)).astype(jnp.bfloat16)
    w_out = (jax.random.normal(shared_keys[6], (OPM_DIM * OPM_DIM, PAIR_DIM), jnp.float32) / OPM_DIM).astype(jnp.bfloat16)
    b_out = (0.25 * NUM_SEQ * jax.random.normal(shared_keys[7], (PAIR_DIM,), jnp.float32)).astype(jnp.bfloat16)
    return {'msa_rep': msa_rep, 'msa_mask': msa_mask, 'pair_rep': pair_rep, 'ln_gamma': ln_gamma, 'ln_beta': ln_beta, 'w_left': w_left, 'b_left': b_left, 'w_right': w_right, 'b_right': b_right, 'w_out': w_out, 'b_out': b_out}


def project_msa(msa_blk, mask_blk, ln_gamma, ln_beta, w_left, b_left, w_right, b_right):
    msa_f32 = msa_blk.astype(jnp.float32)
    mean_x = jnp.mean(msa_f32, axis=-1, keepdims=True)
    centred = msa_f32 - mean_x
    var_x = jnp.mean(centred * centred, axis=-1, keepdims=True)
    normed = (centred * lax.rsqrt(var_x + 1e-5) * ln_gamma.astype(jnp.float32) + ln_beta.astype(jnp.float32)).astype(jnp.bfloat16)
    flat_x = normed.reshape(-1, MSA_DIM)
    keep_col = mask_blk.astype(jnp.float32).reshape(-1, 1)
    left_proj = ((jnp.dot(flat_x, w_left, preferred_element_type=jnp.float32) + b_left.astype(jnp.float32)) * keep_col).astype(jnp.bfloat16)
    right_proj = ((jnp.dot(flat_x, w_right, preferred_element_type=jnp.float32) + b_right.astype(jnp.float32)) * keep_col).astype(jnp.bfloat16)
    out_shape = mask_blk.shape + (OPM_DIM,)
    return left_proj.reshape(out_shape), right_proj.reshape(out_shape)


def reference(msa_rep, msa_mask, pair_rep, ln_gamma, ln_beta, w_left, b_left, w_right, b_right, w_out, b_out):
    seq_blk = 8
    msa_blocks = msa_rep.reshape(NUM_SEQ // seq_blk, seq_blk, NUM_RES, MSA_DIM)
    mask_blocks = msa_mask.reshape(NUM_SEQ // seq_blk, seq_blk, NUM_RES)

    def proj_block(blk_args):
        return project_msa(blk_args[0], blk_args[1], ln_gamma, ln_beta, w_left, b_left, w_right, b_right)

    left_proj, right_proj = lax.map(proj_block, (msa_blocks, mask_blocks))
    left_proj = left_proj.reshape(NUM_SEQ, NUM_RES, OPM_DIM)
    right_f32 = right_proj.reshape(NUM_SEQ, NUM_RES, OPM_DIM).astype(jnp.float32)
    mask_f32 = msa_mask.astype(jnp.float32)
    row_blk = math.gcd(NUM_RES, 2 ** int(math.log2(max(1, 2 ** 24 // (NUM_RES * OPM_DIM * OPM_DIM)))))
    row_count = NUM_RES // row_blk
    left_rows = jnp.moveaxis(left_proj.reshape(NUM_SEQ, row_count, row_blk, OPM_DIM), 1, 0)
    mask_rows = jnp.moveaxis(mask_f32.reshape(NUM_SEQ, row_count, row_blk), 1, 0)
    pair_rows = pair_rep.reshape(row_count, row_blk, NUM_RES, PAIR_DIM)
    bias_out = b_out.astype(jnp.float32)

    def row_block(blk_args):
        left_blk, mask_blk, pair_blk = blk_args
        outer_blk = jnp.einsum('sic,sjd->ijcd', left_blk.astype(jnp.float32), right_f32).astype(jnp.bfloat16)
        summed = jnp.dot(outer_blk.reshape(row_blk * NUM_RES, OPM_DIM * OPM_DIM), w_out, preferred_element_type=jnp.float32).reshape(row_blk, NUM_RES, PAIR_DIM)
        pair_norm = jnp.einsum('si,sj->ij', mask_blk, mask_f32)
        return pair_blk + (summed + bias_out) / (1e-3 + pair_norm)[:, :, None]

    pair_out = lax.map(row_block, (left_rows, mask_rows, pair_rows)).reshape(NUM_RES, NUM_RES, PAIR_DIM)
    return pair_out, msa_rep
```

```python
import functools

import jax
import jax.numpy as jnp
from jax import lax
from jax.experimental import pallas as pl
from jax.experimental.pallas import tpu as pltpu
from jax.sharding import PartitionSpec as P

LN_EPS = 1e-5
NORM_EPS = 1e-3
MESH = pl.DeviceIdType.MESH
F32 = jnp.float32
BF16 = jnp.bfloat16


def kernel(
    n_y, n_dap,
    m_hbm, mask_ref, z_hbm, gamma_ref, beta_ref, wl_ref, bl_ref, wr_ref, br_ref, wo_ref, bo_ref,
    pair_ref, msa_ref,
    m_v, y_s, b_all, o_s, w_s, w_perm, lhs_s, norm_s,
    m_sem, z_sem, own_sem, m_send, m_recv,
    sx, sy, rx, ry, s2a, s2b, r2a, r2b,
    sp0, spx, spy, sp2a, sp2b, rp0, rpx, rpy, rp2a, rp2b,
):
    n_x = n_dap // 2
    n_dev = n_y * n_dap
    n_seq, rows, chans = m_v.shape
    seq_own = n_seq // n_dev
    opm = wl_ref.shape[0]
    n_res = mask_ref.shape[1]
    half = rows * opm // 2
    y = lax.axis_index("outer")
    d = lax.axis_index("dap")
    x, c = d // 2, d % 2
    me = y * n_dap + d

    def dev(dy, dx, dc):
        return {"outer": (y + dy) % n_y, "dap": ((x + dx) % n_x) * 2 + (c + dc) % 2}

    def slot(dy, dx, dc):
        return ((y + n_y - dy) % n_y) * n_dap + ((x + n_x - dx) % n_x) * 2 + (c + dc) % 2

    def remote(src, dst, send, recv, where):
        return pltpu.make_async_remote_copy(
            src_ref=src, dst_ref=dst, send_sem=send, recv_sem=recv, device_id=where, device_id_type=MESH
        )

    offsets = [(dy, dx, dc) for dx in range(n_x) for dy in range(n_y) for dc in range(2) if dy or dx or dc]

    m_in = pltpu.make_async_copy(m_hbm, m_v, m_sem)
    m_in.start()
    z_in = pltpu.make_async_copy(z_hbm, pair_ref, z_sem)
    z_in.start()
    barrier = pltpu.get_barrier_semaphore()
    for off in offsets:
        pl.semaphore_signal(barrier, inc=1, device_id=dev(*off), device_id_type=MESH)

    w_s[...] = wo_ref[...].astype(F32)
    for e in range(opm):
        w_perm[e * opm:(e + 1) * opm, :] = w_s[pl.ds(e, opm, stride=opm), :].astype(BF16)

    mask_b = mask_ref[...].astype(F32).astype(BF16)
    row_of = lax.broadcasted_iota(jnp.int32, (n_res, rows * opm), 0)
    col_of = lax.broadcasted_iota(jnp.int32, (n_res, rows * opm), 1)
    pick = jnp.where(row_of == me * rows + col_of // opm, 1.0, 0.0).astype(BF16)
    mask_own = jnp.dot(mask_b, pick, preferred_element_type=F32)
    norm_s[...] = NORM_EPS + lax.dot_general(
        mask_b, mask_own.astype(BF16), (((0,), (0,)), ((), ())), preferred_element_type=F32
    )

    w_both = jnp.concatenate([wl_ref[...], wr_ref[...]], axis=0)
    b_both = jnp.concatenate([bl_ref[...].astype(F32), br_ref[...].astype(F32)]).reshape(1, 2 * opm)
    gamma = gamma_ref[...].astype(F32).reshape(1, chans)
    beta = beta_ref[...].astype(F32).reshape(1, chans)
    m_in.wait()

    seq_step = 32

    def norm_step(k, carry):
        v = m_v[pl.ds(k * seq_step, seq_step)].astype(F32).reshape(seq_step * rows, chans)
        mean = jnp.mean(v, axis=-1, keepdims=True)
        cen = v - mean
        var = jnp.mean(cen * cen, axis=-1, keepdims=True)
        xn = (cen * lax.rsqrt(var + LN_EPS) * gamma + beta).astype(BF16)
        out = lax.dot_general(xn, w_both, (((1,), (1,)), ((), ())), preferred_element_type=F32) + b_both
        y_s[pl.ds(k * seq_step * rows, seq_step * rows), :] = out
        return carry

    lax.fori_loop(0, n_seq // seq_step, norm_step, 0)

    ys = [y_s[pl.ds(r, n_seq, stride=rows), :] for r in range(rows)]
    a_own = (jnp.concatenate([t[:, :opm] for t in ys], axis=1) * mask_own).astype(BF16)
    b_own = jnp.concatenate([t[:, opm:] for t in ys], axis=1) * mask_own
    b_all[me] = b_own.T.astype(BF16)

    pl.semaphore_wait(barrier, n_dev - 1)

    mine = b_all.at[me]
    sends = []

    def go(copy):
        copy.start()
        sends.append(copy)

    order_x = [1, n_x - 1] + list(range(2, n_x - 1))
    order_y = [1, n_y - 1] + list(range(2, n_y - 1))
    for k in order_x:
        go(remote(mine, mine, sx.at[k], rx.at[k], dev(0, k, 0)))
    for k in order_y:
        go(remote(mine, mine, sy.at[k], ry.at[k], dev(k, 0, 0)))
    go(remote(mine, mine, sp0, rp0, dev(0, 0, 1)))

    keep = pltpu.make_async_copy(m_v.at[pl.ds(me * seq_own, seq_own)], msa_ref.at[:, me], own_sem)
    keep.start()
    m_copies = []
    for i, off in enumerate(offsets):
        to = dev(*off)
        p = to["outer"] * n_dap + to["dap"]
        copy = remote(m_v.at[pl.ds(p * seq_own, seq_own)], msa_ref.at[:, me], m_send.at[i], m_recv.at[i], to)
        go(copy)
        m_copies.append(copy)

    def lower(ref):
        return ref.at[pl.ds(0, half)]

    def upper(ref):
        return ref.at[pl.ds(half, half)]

    def wait_in(ref, sem):
        remote(ref, ref, sem, sem, dev(0, 0, 1)).wait_recv()

    for k in order_x:
        got = b_all.at[slot(0, k, 0)]
        wait_in(got, rx.at[k])
        for j in order_y:
            go(remote(lower(got), lower(got), s2a.at[k, j], r2a.at[k, j], dev(j, 0, 0)))
        go(remote(got, got, spx.at[k], rpx.at[k], dev(0, 0, 1)))
    for j in order_y:
        got = b_all.at[slot(j, 0, 0)]
        wait_in(got, ry.at[j])
        for k in order_x:
            go(remote(upper(got), upper(got), s2b.at[k, j], r2b.at[k, j], dev(0, k, 0)))
        go(remote(got, got, spy.at[j], rpy.at[j], dev(0, 0, 1)))

    bias_out = bo_ref[...].astype(F32).reshape(1, -1)
    z_in.wait()
    line = n_dap * rows

    def pair_line(yl):
        b_line = b_all[pl.ds(yl * n_dap, n_dap)].reshape(line * opm, n_seq)
        o_s[...] = jnp.dot(b_line, a_own, preferred_element_type=F32)
        per = 128 // opm
        for g in range(opm // per):
            parts = [o_s[pl.ds(g * per + q, line, stride=opm), :] for q in range(per)]
            for i in range(rows):
                piece = jnp.concatenate([t[:, i * opm:(i + 1) * opm] for t in parts], axis=1)
                lhs_s[i * line:(i + 1) * line, g * 128:(g + 1) * 128] = piece.astype(BF16)
        res = jnp.dot(lhs_s[...], w_perm[...], preferred_element_type=F32) + bias_out
        at = pl.ds(pl.multiple_of(yl * line, line), line)
        count = norm_s[at, :]
        for i in range(rows):
            pair_ref[i, at, :] += res[i * line:(i + 1) * line] / count[:, i * opm:i * opm + 1]

    wait_in(mine, rp0)
    for k in order_x:
        wait_in(mine, rpx.at[k])
    pair_line(y)

    for j in order_y:
        for k in order_x:
            got = b_all.at[slot(j, k, 0)]
            wait_in(lower(got), r2a.at[k, j])
            go(remote(lower(got), lower(got), sp2a.at[k, j], rp2a.at[k, j], dev(0, 0, 1)))
            wait_in(upper(got), r2b.at[k, j])
            go(remote(upper(got), upper(got), sp2b.at[k, j], rp2b.at[k, j], dev(0, 0, 1)))
    for j in order_y:
        wait_in(mine, rpy.at[j])
        for k in order_x:
            wait_in(lower(mine), rp2a.at[k, j])
            wait_in(upper(mine), rp2b.at[k, j])
        pair_line((y + n_y - j) % n_y)

    for copy in m_copies:
        copy.wait_recv()
    for copy in sends:
        copy.wait_send()
    keep.wait()


def solution(mesh):
    n_y, n_dap = mesh.shape["outer"], mesh.shape["dap"]
    n_x, n_dev = n_dap // 2, n_y * n_dap
    dap_axes = ("outer", "dap")
    group_axes = ("data", "outer", "dap")

    def local_step(msa, mask, pair, gamma, beta, w_left, b_left, w_right, b_right, w_out, b_out):
        n_seq, rows, chans = msa.shape
        n_res = mask.shape[1]
        opm = w_left.shape[1]
        pair_dim = w_out.shape[1]
        seq_own = n_seq // n_dev
        line = n_dap * rows
        dma = pltpu.SemaphoreType.DMA
        any_spec = pl.BlockSpec(memory_space=pl.ANY)
        vmem = pl.BlockSpec(memory_space=pltpu.VMEM)
        pair_out, msa_out = pl.pallas_call(
            functools.partial(kernel, n_y, n_dap),
            out_shape=(
                jax.ShapeDtypeStruct(pair.shape, F32),
                jax.ShapeDtypeStruct((seq_own, n_dev, rows, chans), BF16),
            ),
            in_specs=[any_spec, vmem, any_spec] + [vmem] * 8,
            out_specs=(vmem, any_spec),
            scratch_shapes=[
                pltpu.VMEM((n_seq, rows, chans), BF16),
                pltpu.VMEM((n_seq * rows, 2 * opm), F32),
                pltpu.VMEM((n_dev, rows * opm, n_seq), BF16),
                pltpu.VMEM((line * opm, rows * opm), F32),
                pltpu.VMEM((opm * opm, pair_dim), F32),
                pltpu.VMEM((opm * opm, pair_dim), BF16),
                pltpu.VMEM((rows * line, opm * opm), BF16),
                pltpu.VMEM((n_res, rows * opm), F32),
                dma, dma, dma, dma((n_dev - 1,)), dma((n_dev - 1,)),
                dma((n_x,)), dma((n_y,)), dma((n_x,)), dma((n_y,)),
                dma((n_x, n_y)), dma((n_x, n_y)), dma((n_x, n_y)), dma((n_x, n_y)),
                dma, dma((n_x,)), dma((n_y,)), dma((n_x, n_y)), dma((n_x, n_y)),
                dma, dma((n_x,)), dma((n_y,)), dma((n_x, n_y)), dma((n_x, n_y)),
            ],
            compiler_params=pltpu.CompilerParams(collective_id=0, has_side_effects=True),
        )(msa, mask, pair, gamma, beta, w_left.T, b_left, w_right.T, b_right, w_out, b_out)
        return pair_out, msa_out.reshape(seq_own, n_dev * rows, chans)

    return jax.shard_map(
        local_step, mesh=mesh,
        in_specs=(P("data", dap_axes, None), P("data", None), P(group_axes, None, None)) + (P(),) * 8,
        out_specs=(P(group_axes, None, None), P(group_axes, None, None)), check_vma=False,
    )
```

```python
import functools

import jax
import jax.numpy as jnp
from jax import lax
from jax.experimental import pallas as pl
from jax.experimental.pallas import tpu as pltpu
from jax.sharding import PartitionSpec as P

LN_EPS = 1e-5
NORM_EPS = 1e-3
MESH = pl.DeviceIdType.MESH
F32 = jnp.float32
BF16 = jnp.bfloat16
LN_CHUNKS = 4
EARLY_AT = 0
EARLY = 0
MIDDLE = 31


def kernel(
    n_y, n_dap,
    m_hbm, mask_hbm, z_hbm, gamma_hbm, beta_hbm, wl_hbm, bl_hbm, wr_hbm, br_hbm, wo_hbm, bo_hbm,
    pair_ref, msa_ref,
    m_v, mask_v, gamma_v, beta_v, wl_v, bl_v, wr_v, br_v, wo_v, bo_v,
    m_got, y_s, a_all, b_col, o_s, w_s, w_perm, lhs_s, den_s, r_send, r_got,
    in_sem, m_sem, own_sem, m_send, m_recv,
    a_send, a_recv, b_send, b_recv, p_send, p_recv, r_ssem, r_rsem,
):
    n_x = n_dap // 2
    n_dev = n_y * n_dap
    n_seq, rows, chans = m_v.shape
    seq_own = n_seq // n_dev
    opm = wl_v.shape[0]
    n_res = mask_v.shape[1]
    group = 2 * rows
    line = n_y * group
    y = lax.axis_index("outer")
    d = lax.axis_index("dap")
    x, c = d // 2, d % 2
    me = y * n_dap + d

    def dev(dy, dx, dc):
        return {"outer": (y + dy) % n_y, "dap": ((x + dx) % n_x) * 2 + (c + dc) % 2}

    def remote(src, dst, send, recv, where):
        return pltpu.make_async_remote_copy(
            src_ref=src, dst_ref=dst, send_sem=send, recv_sem=recv, device_id=where, device_id_type=MESH
        )

    def wait_in(ref, sem):
        remote(ref, ref, sem, sem, dev(0, 0, 1)).wait_recv()

    sends = []

    def go(copy):
        copy.start()
        sends.append(copy)

    order_x = [1, n_x - 1] + list(range(2, n_x - 1))
    order_y = [1, n_y - 1] + list(range(2, n_y - 1))
    offsets = [(dy, dx, dc) for dx in range(n_x) for dy in range(n_y) for dc in range(2) if dy or dx or dc]

    piece = n_seq // LN_CHUNKS
    m_in = []
    for k in range(LN_CHUNKS):
        part = pl.ds(k * piece, piece)
        m_in.append(pltpu.make_async_copy(m_hbm.at[part], m_v.at[part], m_sem.at[k]))
    pairs = [
        (gamma_hbm, gamma_v), (beta_hbm, beta_v), (wl_hbm, wl_v), (wr_hbm, wr_v), (bl_hbm, bl_v), (br_hbm, br_v),
        (mask_hbm, mask_v), (wo_hbm, wo_v), (bo_hbm, bo_v), (z_hbm, pair_ref),
    ]
    small_in = [pltpu.make_async_copy(src, dst, in_sem.at[i]) for i, (src, dst) in enumerate(pairs)]
    for copy in small_in[:2] + m_in[:1] + small_in[2:6] + m_in[1:] + small_in[6:]:
        copy.start()
    barrier = pltpu.get_barrier_semaphore()
    for off in offsets:
        pl.semaphore_signal(barrier, inc=1, device_id=dev(*off), device_id_type=MESH)

    m_copies = []
    for i, off in enumerate(offsets):
        to = dev(*off)
        p = to["outer"] * n_dap + to["dap"]
        m_copies.append(
            remote(m_v.at[pl.ds(p * seq_own, seq_own)], m_got.at[:, me], m_send.at[i], m_recv.at[i], to)
        )

    for copy in small_in[:6]:
        copy.wait()
    w_both = jnp.concatenate([wl_v[...], wr_v[...]], axis=0)
    b_both = jnp.concatenate([bl_v[...].astype(F32), br_v[...].astype(F32)]).reshape(1, 2 * opm)
    gamma = gamma_v[...].astype(F32).reshape(1, chans)
    beta = beta_v[...].astype(F32).reshape(1, chans)

    def normalise(k):
        if k < EARLY_AT or not EARLY:
            m_in[k].wait()
        v = m_v[k * piece:(k + 1) * piece].astype(F32).reshape(piece * rows, chans)
        mean = jnp.mean(v, axis=-1, keepdims=True)
        cen = v - mean
        var = jnp.mean(cen * cen, axis=-1, keepdims=True)
        xn = (cen * lax.rsqrt(var + LN_EPS) * gamma + beta).astype(BF16)
        out = lax.dot_general(xn, w_both, (((1,), (1,)), ((), ())), preferred_element_type=F32) + b_both
        y_s[k * piece * rows:(k + 1) * piece * rows, :] = out

    for k in range(EARLY_AT):
        normalise(k)
    if EARLY:
        for k in range(EARLY_AT, LN_CHUNKS):
            m_in[k].wait()
        pl.semaphore_wait(barrier, n_dev - 1)
        for copy in m_copies[:EARLY]:
            go(copy)


    for k in range(EARLY_AT, LN_CHUNKS):
        normalise(k)

    small_in[6].wait()
    mask_b = mask_v[...].astype(F32).astype(BF16)
    row_of = lax.broadcasted_iota(jnp.int32, (n_res, rows * opm), 0)
    col_of = lax.broadcasted_iota(jnp.int32, (n_res, rows * opm), 1)
    pick = jnp.where(row_of == me * rows + col_of // opm, 1.0, 0.0).astype(BF16)
    mask_own = jnp.dot(mask_b, pick, preferred_element_type=F32)

    ys = [y_s[pl.ds(r, n_seq, stride=rows), :] for r in range(rows)]
    a_all[0] = (jnp.concatenate([t[:, :opm] for t in ys], axis=1) * mask_own).astype(BF16)
    b_own = jnp.concatenate([t[:, opm:] for t in ys], axis=1) * mask_own
    b_col[y * 2 + c] = b_own.T.astype(BF16)

    if not EARLY:
        pl.semaphore_wait(barrier, n_dev - 1)

    mine = b_col.at[y * 2 + c]
    go(remote(mine, mine, p_send.at[0], p_recv.at[0], dev(0, 0, 1)))
    for k in order_y:
        go(remote(mine, mine, b_send.at[k], b_recv.at[k], dev(k, 0, 0)))
    for k in order_x:
        go(remote(a_all.at[0], a_all.at[k], a_send.at[k], a_recv.at[k], dev(0, k, 0)))
    keep = pltpu.make_async_copy(m_v.at[pl.ds(me * seq_own, seq_own)], m_got.at[:, me], own_sem)
    keep.start()
    for copy in m_copies[EARLY:MIDDLE]:
        go(copy)

    for copy in small_in[7:]:
        copy.wait()
    w_s[...] = wo_v[...].astype(F32)
    for e in range(opm):
        w_perm[e * opm:(e + 1) * opm, :] = w_s[pl.ds(e, opm, stride=opm), :].astype(BF16)
    count = lax.dot_general(
        mask_b, mask_own.astype(BF16), (((0,), (0,)), ((), ())), preferred_element_type=F32
    )
    for i in range(rows):
        den_s[i] = jnp.broadcast_to(NORM_EPS + count[:, i * opm:i * opm + 1], den_s.shape[1:])
    bias_out = bo_v[...].astype(F32).reshape(1, -1)

    for k in order_y:
        got = b_col.at[((y + n_y - k) % n_y) * 2 + c]
        wait_in(got, b_recv.at[k])
        go(remote(got, got, p_send.at[k], p_recv.at[k], dev(0, 0, 1)))
    for k in range(n_y):
        wait_in(mine, p_recv.at[k])

    per = 128 // opm

    def outer(k):
        b_line = b_col[...].reshape(line * opm, n_seq)
        o_s[...] = jnp.dot(b_line, a_all[k], preferred_element_type=F32)
        for g in range(opm // per):
            parts = [o_s[pl.ds(g * per + q, line, stride=opm), :] for q in range(per)]
            for i in range(rows):
                block = jnp.concatenate([t[:, i * opm:(i + 1) * opm] for t in parts], axis=1)
                lhs_s[i * line:(i + 1) * line, g * 128:(g + 1) * 128] = block.astype(BF16)
        return jnp.dot(lhs_s[...], w_perm[...], preferred_element_type=F32)

    def finish(res, xs):
        for i in range(rows):
            for t in range(n_y):
                at = pl.ds(pl.multiple_of(t * n_x * group + xs * group, group), group)
                part = res[(i * n_y + t) * group:(i * n_y + t + 1) * group]
                pair_ref[i, at, :] += (part + bias_out) / den_s[i, at, :]

    for k in order_x[2:] + order_x[:2]:
        wait_in(a_all.at[k], a_recv.at[k])
        r_send[k] = outer(k)
        go(remote(r_send.at[k], r_got.at[k], r_ssem.at[k], r_rsem.at[k], dev(0, n_x - k, 0)))
    for copy in m_copies[MIDDLE:]:
        go(copy)
    finish(outer(0), x)
    for k in order_x[2:] + order_x[:2]:
        wait_in(r_got.at[k], r_rsem.at[k])
        finish(r_got[k], (x + k) % n_x)

    for copy in m_copies:
        copy.wait_recv()
    keep.wait()
    for s in range(seq_own):
        msa_ref[s] = m_got[s].astype(F32).reshape(n_res, chans).astype(BF16)
    for copy in sends:
        copy.wait_send()


def solution(mesh):
    n_y, n_dap = mesh.shape["outer"], mesh.shape["dap"]
    n_x, n_dev = n_dap // 2, n_y * n_dap
    dap_axes = ("outer", "dap")
    group_axes = ("data", "outer", "dap")

    def local_step(msa, mask, pair, gamma, beta, w_left, b_left, w_right, b_right, w_out, b_out):
        n_seq, rows, chans = msa.shape
        n_res = mask.shape[1]
        opm = w_left.shape[1]
        pair_dim = w_out.shape[1]
        seq_own = n_seq // n_dev
        line = n_y * 2 * rows
        dma = pltpu.SemaphoreType.DMA
        vmem = pl.BlockSpec(memory_space=pltpu.VMEM)
        ins = (msa, mask, pair, gamma, beta, w_left.T, b_left, w_right.T, b_right, w_out, b_out)
        return pl.pallas_call(
            functools.partial(kernel, n_y, n_dap),
            out_shape=(
                pltpu.VMEM(pair.shape, F32),
                pltpu.VMEM((seq_own, n_dev * rows, chans), BF16),
            ),
            in_specs=[pl.BlockSpec(memory_space=pl.ANY)] * len(ins),
            out_specs=(vmem, vmem),
            scratch_shapes=[pltpu.VMEM(v.shape, v.dtype) for v in ins[:2] + ins[3:]] + [
                pltpu.VMEM((seq_own, n_dev, rows, chans), BF16),
                pltpu.VMEM((n_seq * rows, 2 * opm), F32),
                pltpu.VMEM((n_x, n_seq, rows * opm), BF16),
                pltpu.VMEM((n_y * 2, rows * opm, n_seq), BF16),
                pltpu.VMEM((line * opm, rows * opm), F32),
                pltpu.VMEM((opm * opm, pair_dim), F32),
                pltpu.VMEM((opm * opm, pair_dim), BF16),
                pltpu.VMEM((rows * line, opm * opm), BF16),
                pltpu.VMEM((rows, n_res, pair_dim), F32),
                pltpu.VMEM((n_x, rows * line, pair_dim), F32),
                pltpu.VMEM((n_x, rows * line, pair_dim), F32),
                dma((10,)), dma((LN_CHUNKS,)), dma, dma((n_dev - 1,)), dma((n_dev - 1,)),
                dma((n_x,)), dma((n_x,)), dma((n_y,)), dma((n_y,)), dma((n_y,)), dma((n_y,)), dma((n_x,)), dma((n_x,)),
            ],
            compiler_params=pltpu.CompilerParams(collective_id=0, has_side_effects=True),
        )(*ins)

    return jax.shard_map(
        local_step, mesh=mesh,
        in_specs=(P("data", dap_axes, None), P("data", None), P(group_axes, None, None)) + (P(),) * 8,
        out_specs=(P(group_axes, None, None), P(group_axes, None, None)), check_vma=False,
    )
```

```python
import functools

import jax
import jax.numpy as jnp
from jax import lax
from jax.experimental import pallas as pl
from jax.experimental.pallas import tpu as pltpu
from jax.sharding import PartitionSpec as P

LN_EPS = 1e-5
NORM_EPS = 1e-3
MESH = pl.DeviceIdType.MESH
F32 = jnp.float32
BF16 = jnp.bfloat16
LN_CHUNKS = 1
M_FIRST = 0
M_STEPS = (31, 0, 0)


def kernel(
    n_y, n_dap,
    m_hbm, mask_hbm, z_hbm, gamma_hbm, beta_hbm, wl_hbm, bl_hbm, wr_hbm, br_hbm, wo_hbm, bo_hbm,
    pair_ref, msa_ref,
    m_v, mask_v, gamma_v, beta_v, wl_v, bl_v, wr_v, br_v, wo_v, bo_v,
    m_got, y_s, a_all, b_row, o_s, w_s, w_perm, lhs_s, den_s, r_send, r_got,
    in_sem, m_sem, own_sem, m_send, m_recv,
    a_send, a_recv, b_send, b_recv, p_send, p_recv, r_ssem, r_rsem,
):
    n_x = n_dap // 2
    n_dev = n_y * n_dap
    n_seq, rows, chans = m_v.shape
    seq_own = n_seq // n_dev
    opm = wl_v.shape[0]
    n_res = mask_v.shape[1]
    line = n_dap * rows
    y = lax.axis_index("outer")
    d = lax.axis_index("dap")
    x, c = d // 2, d % 2
    me = y * n_dap + d

    def dev(dy, dx, dc):
        return {"outer": (y + dy) % n_y, "dap": ((x + dx) % n_x) * 2 + (c + dc) % 2}

    def remote(src, dst, send, recv, where):
        return pltpu.make_async_remote_copy(
            src_ref=src, dst_ref=dst, send_sem=send, recv_sem=recv, device_id=where, device_id_type=MESH
        )

    def wait_in(ref, sem):
        remote(ref, ref, sem, sem, dev(0, 0, 1)).wait_recv()

    sends = []

    def go(copy):
        copy.start()
        sends.append(copy)

    order_x = list(range(2, n_x - 1)) + [1, n_x - 1]
    order_y = list(range(2, n_y - 1)) + [1, n_y - 1]
    offsets = [(dy, dx, dc) for dx in range(n_x) for dy in range(n_y) for dc in range(2) if dy or dx or dc]

    offsets.sort(key=lambda o: -(min(o[0], n_y - o[0]) + min(o[1], n_x - o[1])))

    piece = n_seq // LN_CHUNKS
    m_in = []
    for k in range(LN_CHUNKS):
        part = pl.ds(k * piece, piece)
        m_in.append(pltpu.make_async_copy(m_hbm.at[part], m_v.at[part], m_sem.at[k]))
    pairs = [
        (gamma_hbm, gamma_v), (beta_hbm, beta_v), (wl_hbm, wl_v), (wr_hbm, wr_v), (bl_hbm, bl_v), (br_hbm, br_v),
        (mask_hbm, mask_v), (wo_hbm, wo_v), (bo_hbm, bo_v), (z_hbm, pair_ref),
    ]
    small_in = [pltpu.make_async_copy(src, dst, in_sem.at[i]) for i, (src, dst) in enumerate(pairs)]
    for copy in small_in[:2] + m_in[:1] + small_in[2:6] + m_in[1:] + small_in[6:]:
        copy.start()
    barrier = pltpu.get_barrier_semaphore()
    for off in offsets:
        pl.semaphore_signal(barrier, inc=1, device_id=dev(*off), device_id_type=MESH)

    m_copies = []
    for i, off in enumerate(offsets):
        to = dev(*off)
        p = to["outer"] * n_dap + to["dap"]
        m_copies.append(
            remote(m_v.at[pl.ds(p * seq_own, seq_own)], m_got.at[me], m_send.at[i], m_recv.at[i], to)
        )

    for copy in small_in[:6]:
        copy.wait()
    w_both = jnp.concatenate([wl_v[...], wr_v[...]], axis=0)
    b_both = jnp.concatenate([bl_v[...].astype(F32), br_v[...].astype(F32)]).reshape(1, 2 * opm)
    gamma = gamma_v[...].astype(F32).reshape(1, chans)
    beta = beta_v[...].astype(F32).reshape(1, chans)

    def normalise(k):
        m_in[k].wait()
        v = m_v[k * piece:(k + 1) * piece].astype(F32).reshape(piece * rows, chans)
        mean = jnp.mean(v, axis=-1, keepdims=True)
        cen = v - mean
        var = jnp.mean(cen * cen, axis=-1, keepdims=True)
        xn = (cen * lax.rsqrt(var + LN_EPS) * gamma + beta).astype(BF16)
        out = lax.dot_general(xn, w_both, (((1,), (1,)), ((), ())), preferred_element_type=F32) + b_both
        y_s[k * piece * rows:(k + 1) * piece * rows, :] = out

    for k in range(LN_CHUNKS):
        normalise(k)

    small_in[6].wait()
    mask_b = mask_v[...].astype(F32).astype(BF16)
    row_of = lax.broadcasted_iota(jnp.int32, (n_res, rows * opm), 0)
    col_of = lax.broadcasted_iota(jnp.int32, (n_res, rows * opm), 1)
    pick = jnp.where(row_of == me * rows + col_of // opm, 1.0, 0.0).astype(BF16)
    mask_own = jnp.dot(mask_b, pick, preferred_element_type=F32)

    ys = [y_s[pl.ds(r, n_seq, stride=rows), :] for r in range(rows)]
    a_all[0] = (jnp.concatenate([t[:, :opm] for t in ys], axis=1) * mask_own).astype(BF16)
    b_own = jnp.concatenate([t[:, opm:] for t in ys], axis=1) * mask_own
    b_row[d] = b_own.T.astype(BF16)

    left = list(m_copies)

    def send_m(count):
        for _ in range(min(count, len(left))):
            go(left.pop(0))

    pl.semaphore_wait(barrier, n_dev - 1)
    send_m(M_FIRST)
    mine = b_row.at[d]
    go(remote(mine, mine, p_send.at[0], p_recv.at[0], dev(0, 0, 1)))
    for kx, ky in zip(order_x, order_y, strict=True):
        go(remote(mine, mine, b_send.at[kx], b_recv.at[kx], dev(0, kx, 0)))
        go(remote(a_all.at[0], a_all.at[ky], a_send.at[ky], a_recv.at[ky], dev(ky, 0, 0)))
    keep = pltpu.make_async_copy(m_v.at[pl.ds(me * seq_own, seq_own)], m_got.at[me], own_sem)
    keep.start()
    send_m(M_STEPS[0])

    for copy in small_in[7:]:
        copy.wait()
    w_s[...] = wo_v[...].astype(F32)
    for e in range(opm):
        w_perm[e * opm:(e + 1) * opm, :] = w_s[pl.ds(e, opm, stride=opm), :].astype(BF16)
    count = lax.dot_general(
        mask_b, mask_own.astype(BF16), (((0,), (0,)), ((), ())), preferred_element_type=F32
    )
    for i in range(rows):
        den_s[i] = jnp.broadcast_to(NORM_EPS + count[:, i * opm:i * opm + 1], den_s.shape[1:])
    bias_out = bo_v[...].astype(F32).reshape(1, -1)

    for k in order_x:
        got = b_row.at[((x + n_x - k) % n_x) * 2 + c]
        wait_in(got, b_recv.at[k])
        go(remote(got, got, p_send.at[k], p_recv.at[k], dev(0, 0, 1)))
    send_m(M_STEPS[1])
    for k in range(n_x):
        wait_in(mine, p_recv.at[k])

    per = 128 // opm

    def outer(k):
        b_line = b_row[...].reshape(line * opm, n_seq)
        o_s[...] = jnp.dot(b_line, a_all[k], preferred_element_type=F32)
        for g in range(opm // per):
            parts = [o_s[pl.ds(g * per + q, line, stride=opm), :] for q in range(per)]
            for i in range(rows):
                block = jnp.concatenate([t[:, i * opm:(i + 1) * opm] for t in parts], axis=1)
                lhs_s[i * line:(i + 1) * line, g * 128:(g + 1) * 128] = block.astype(BF16)
        return jnp.dot(lhs_s[...], w_perm[...], preferred_element_type=F32)

    def finish(res, ys):
        at = pl.ds(pl.multiple_of(ys * line, line), line)
        for i in range(rows):
            pair_ref[i, at, :] += (res[i * line:(i + 1) * line] + bias_out) / den_s[i, at, :]

    for k in order_y:
        wait_in(a_all.at[k], a_recv.at[k])
        r_send[k] = outer(k)
        go(remote(r_send.at[k], r_got.at[k], r_ssem.at[k], r_rsem.at[k], dev(n_y - k, 0, 0)))
    send_m(M_STEPS[2])
    finish(outer(0), y)
    send_m(len(left))
    for k in order_y:
        wait_in(r_got.at[k], r_rsem.at[k])
        finish(r_got[k], (y + k) % n_y)

    for copy in m_copies:
        copy.wait_recv()
    keep.wait()
    for s in range(seq_own):
        msa_ref[s] = m_got[:, s].astype(F32).reshape(n_res, chans).astype(BF16)
    for copy in sends:
        copy.wait_send()


def store(pair_v, msa_v, pair_ref, msa_ref, sem):
    copies = [pltpu.make_async_copy(pair_v, pair_ref, sem.at[0]), pltpu.make_async_copy(msa_v, msa_ref, sem.at[1])]
    for copy in copies:
        copy.start()
    for copy in copies:
        copy.wait()


def solution(mesh):
    n_y, n_dap = mesh.shape["outer"], mesh.shape["dap"]
    n_x, n_dev = n_dap // 2, n_y * n_dap
    dap_axes = ("outer", "dap")
    group_axes = ("data", "outer", "dap")

    def local_step(msa, mask, pair, gamma, beta, w_left, b_left, w_right, b_right, w_out, b_out):
        n_seq, rows, chans = msa.shape
        n_res = mask.shape[1]
        opm = w_left.shape[1]
        pair_dim = w_out.shape[1]
        seq_own = n_seq // n_dev
        line = n_dap * rows
        dma = pltpu.SemaphoreType.DMA
        vmem = pl.BlockSpec(memory_space=pltpu.VMEM)
        ins = (msa, mask, pair, gamma, beta, w_left.T, b_left, w_right.T, b_right, w_out, b_out)
        got = pl.pallas_call(
            functools.partial(kernel, n_y, n_dap),
            out_shape=(
                pltpu.VMEM(pair.shape, F32),
                pltpu.VMEM((seq_own, n_dev * rows, chans), BF16),
            ),
            in_specs=[pl.BlockSpec(memory_space=pl.ANY)] * len(ins),
            out_specs=(vmem, vmem),
            scratch_shapes=[pltpu.VMEM(v.shape, v.dtype) for v in ins[:2] + ins[3:]] + [
                pltpu.VMEM((n_dev, seq_own, rows, chans), BF16),
                pltpu.VMEM((n_seq * rows, 2 * opm), F32),
                pltpu.VMEM((n_y, n_seq, rows * opm), BF16),
                pltpu.VMEM((n_dap, rows * opm, n_seq), BF16),
                pltpu.VMEM((line * opm, rows * opm), F32),
                pltpu.VMEM((opm * opm, pair_dim), F32),
                pltpu.VMEM((opm * opm, pair_dim), BF16),
                pltpu.VMEM((rows * line, opm * opm), BF16),
                pltpu.VMEM((rows, n_res, pair_dim), F32),
                pltpu.VMEM((n_y, rows * line, pair_dim), F32),
                pltpu.VMEM((n_y, rows * line, pair_dim), F32),
                dma((10,)), dma((LN_CHUNKS,)), dma, dma((n_dev - 1,)), dma((n_dev - 1,)),
                dma((n_y,)), dma((n_y,)), dma((n_x,)), dma((n_x,)), dma((n_x,)), dma((n_x,)), dma((n_y,)), dma((n_y,)),
            ],
            compiler_params=pltpu.CompilerParams(collective_id=0, has_side_effects=True),
        )(*ins)
        return pl.pallas_call(
            store,
            out_shape=tuple(jax.ShapeDtypeStruct(v.shape, v.dtype) for v in got),
            in_specs=[pl.BlockSpec(memory_space=pl.ANY)] * 2,
            out_specs=(pl.BlockSpec(memory_space=pl.ANY),) * 2,
            scratch_shapes=[dma((2,))],
            compiler_params=pltpu.CompilerParams(vmem_limit_bytes=4 * 1024 * 1024),
        )(*got)

    return jax.shard_map(
        local_step, mesh=mesh,
        in_specs=(P("data", dap_axes, None), P("data", None), P(group_axes, None, None)) + (P(),) * 8,
        out_specs=(P(group_axes, None, None), P(group_axes, None, None)), check_vma=False,
    )
```

```python
import functools

import jax
import jax.numpy as jnp
from jax import lax
from jax.experimental import pallas as pl
from jax.experimental.pallas import tpu as pltpu
from jax.sharding import PartitionSpec as P

LN_EPS = 1e-5
NORM_EPS = 1e-3
MESH = pl.DeviceIdType.MESH
F32 = jnp.float32
BF16 = jnp.bfloat16
LN_CHUNKS = 1
M_FIRST = 0
M_STEPS = (31, 0, 0)


def kernel(
    n_y, n_dap,
    m_hbm, mask_hbm, z_hbm, gamma_hbm, beta_hbm, wl_hbm, bl_hbm, wr_hbm, br_hbm, wo_hbm, bo_hbm,
    pair_ref, msa_ref,
    m_v, mask_v, gamma_v, beta_v, wl_v, bl_v, wr_v, br_v, wo_v, bo_v,
    m_got, y_s, a_all, b_row, o_s, w_s, w_perm, lhs_s, den_s, r_send, r_got,
    in_sem, m_sem, own_sem, m_send, m_recv,
    a_send, a_recv, b_send, b_recv, p_send, p_recv, r_ssem, r_rsem,
):
    n_x = n_dap // 2
    n_dev = n_y * n_dap
    n_seq, rows, chans = m_v.shape
    seq_own = n_seq // n_dev
    opm = wl_v.shape[0]
    n_res = mask_v.shape[1]
    line = n_x * rows
    y = lax.axis_index("outer")
    d = lax.axis_index("dap")
    x, c = d // 2, d % 2
    me = y * n_dap + d

    ys = [lax.rem(y + k, n_y) for k in range(n_y)]
    xs = [lax.rem(x + k, n_x) for k in range(n_x)]
    cs = [c, 1 - c]

    def dev(dy, dx, dc):
        return {"outer": ys[dy % n_y], "dap": xs[dx % n_x] * 2 + cs[dc]}

    def remote(src, dst, send, recv, where):
        return pltpu.make_async_remote_copy(
            src_ref=src, dst_ref=dst, send_sem=send, recv_sem=recv, device_id=where, device_id_type=MESH
        )

    def wait_in(ref, sem):
        remote(ref, ref, sem, sem, dev(0, 0, 1)).wait_recv()

    sends = []

    def go(copy):
        copy.start()
        sends.append(copy)

    order_x = list(range(2, n_x - 1)) + [1, n_x - 1]
    order_y = list(range(2, n_y - 1)) + [1, n_y - 1]
    offsets = [(dy, dx, dc) for dx in range(n_x) for dy in range(n_y) for dc in range(2) if dy or dx or dc]

    offsets.sort(key=lambda o: (-o[2], -(min(o[0], n_y - o[0]) + min(o[1], n_x - o[1]))))

    piece = n_seq // LN_CHUNKS
    m_in = []
    for k in range(LN_CHUNKS):
        part = pl.ds(k * piece, piece)
        m_in.append(pltpu.make_async_copy(m_hbm.at[part], m_v.at[part], m_sem.at[k]))
    pairs = [
        (gamma_hbm, gamma_v), (beta_hbm, beta_v), (wl_hbm, wl_v), (wr_hbm, wr_v), (bl_hbm, bl_v), (br_hbm, br_v),
        (mask_hbm, mask_v), (wo_hbm, wo_v), (bo_hbm, bo_v), (z_hbm, pair_ref),
    ]
    small_in = [pltpu.make_async_copy(src, dst, in_sem.at[i]) for i, (src, dst) in enumerate(pairs)]
    for copy in small_in[:2] + m_in[:1] + small_in[2:6] + m_in[1:] + small_in[6:]:
        copy.start()
    barrier = pltpu.get_barrier_semaphore()
    for off in offsets:
        pl.semaphore_signal(barrier, inc=1, device_id=dev(*off), device_id_type=MESH)

    m_copies = []
    for i, off in enumerate(offsets):
        to = dev(*off)
        p = to["outer"] * n_dap + to["dap"]
        m_copies.append(
            remote(m_v.at[pl.ds(p * seq_own, seq_own)], m_got.at[me], m_send.at[i], m_recv.at[i], to)
        )

    for copy in small_in[:6]:
        copy.wait()
    w_both = jnp.concatenate([wl_v[...], wr_v[...]], axis=0)
    b_both = jnp.concatenate([bl_v[...].astype(F32), br_v[...].astype(F32)]).reshape(1, 2 * opm)
    gamma = gamma_v[...].astype(F32).reshape(1, chans)
    beta = beta_v[...].astype(F32).reshape(1, chans)

    def normalise(k):
        m_in[k].wait()
        v = m_v[k * piece:(k + 1) * piece].astype(F32).reshape(piece * rows, chans)
        mean = jnp.mean(v, axis=-1, keepdims=True)
        cen = v - mean
        var = jnp.mean(cen * cen, axis=-1, keepdims=True)
        xn = (cen * lax.rsqrt(var + LN_EPS) * gamma + beta).astype(BF16)
        out = lax.dot_general(xn, w_both, (((1,), (1,)), ((), ())), preferred_element_type=F32) + b_both
        y_s[k * piece * rows:(k + 1) * piece * rows, :] = out

    for k in range(LN_CHUNKS):
        normalise(k)

    small_in[6].wait()
    mask_b = mask_v[...].astype(F32).astype(BF16)
    row_of = lax.broadcasted_iota(jnp.int32, (n_res, rows * opm), 0)
    col_of = lax.broadcasted_iota(jnp.int32, (n_res, rows * opm), 1)
    pick = jnp.where(row_of == me * rows + col_of // opm, 1.0, 0.0).astype(BF16)
    mask_own = jnp.dot(mask_b, pick, preferred_element_type=F32)

    proj = [y_s[pl.ds(r, n_seq, stride=rows), :] for r in range(rows)]
    a_all[0] = (jnp.concatenate([t[:, :opm] for t in proj], axis=1) * mask_own).astype(BF16)
    b_own = jnp.concatenate([t[:, opm:] for t in proj], axis=1) * mask_own
    b_row[x] = b_own.T.astype(BF16)

    left = list(m_copies)

    def send_m(count):
        for _ in range(min(count, len(left))):
            go(left.pop(0))

    pl.semaphore_wait(barrier, n_dev - 1)
    send_m(M_FIRST)
    mine = b_row.at[x]
    go(remote(mine, b_row.at[n_x + x], p_send.at[0], p_recv.at[0], dev(0, 0, 1)))
    for kx, ky in zip(order_x, order_y, strict=True):
        go(remote(mine, mine, b_send.at[kx], b_recv.at[kx], dev(0, kx, 0)))
        go(remote(a_all.at[0], a_all.at[ky], a_send.at[ky], a_recv.at[ky], dev(ky, 0, 0)))
    keep = pltpu.make_async_copy(m_v.at[pl.ds(me * seq_own, seq_own)], m_got.at[me], own_sem)
    keep.start()
    send_m(M_STEPS[0])

    for copy in small_in[7:]:
        copy.wait()
    w_s[...] = wo_v[...].astype(F32)
    for e in range(opm):
        w_perm[e * opm:(e + 1) * opm, :] = w_s[pl.ds(e, opm, stride=opm), :].astype(BF16)
    count = lax.dot_general(
        mask_b, mask_own.astype(BF16), (((0,), (0,)), ((), ())), preferred_element_type=F32
    )
    for i in range(rows):
        den_s[i] = jnp.broadcast_to(NORM_EPS + count[:, i * opm:i * opm + 1], den_s.shape[1:])
    bias_out = bo_v[...].astype(F32).reshape(1, -1)

    for k in order_x:
        at = xs[n_x - k]
        got = b_row.at[at]
        wait_in(got, b_recv.at[k])
        go(remote(got, b_row.at[n_x + at], p_send.at[k], p_recv.at[k], dev(0, 0, 1)))
    send_m(M_STEPS[1])

    per = 128 // opm

    def outer(h, slots):
        b_line = b_row[h * n_x:(h + 1) * n_x].reshape(line * opm, n_seq)
        a_pair = jnp.concatenate([a_all[k] for k in slots], axis=1)
        both = jnp.dot(b_line, a_pair, preferred_element_type=F32)
        for t in range(len(slots)):
            o_s[t] = both[:, t * rows * opm:(t + 1) * rows * opm]
        for g in range(opm // per):
            for t in range(len(slots)):
                parts = [o_s[t, pl.ds(g * per + q, line, stride=opm), :].astype(BF16) for q in range(per)]
                for i in range(rows):
                    block = jnp.concatenate([v[:, i * opm:(i + 1) * opm] for v in parts], axis=1)
                    to = (t * rows + i) * line
                    lhs_s[to:to + line, g * 128:(g + 1) * 128] = block.astype(BF16)
        res = jnp.dot(lhs_s[...], w_perm[...], preferred_element_type=F32)
        return [res[t * rows * line:(t + 1) * rows * line] for t in range(len(slots))]

    def finish(h, res, row):
        for i in range(rows):
            for t in range(n_x):
                at = pl.ds((row * n_x + t) * 2 * rows + cs[h] * rows, rows)
                part = res[(i * n_x + t) * rows:(i * n_x + t + 1) * rows]
                pair_ref[i, at, :] += (part + bias_out) / den_s[i, at, :]

    slots = order_y + [0]
    own = []
    for h in range(2):
        if h == 1:
            for k in range(n_x):
                wait_in(mine, p_recv.at[k])
        for n in range(0, n_y, 2):
            pick_two = slots[n:n + 2]
            if h == 0:
                for k in pick_two:
                    if k:
                        wait_in(a_all.at[k], a_recv.at[k])
            for k, res in zip(pick_two, outer(h, pick_two), strict=True):
                r_send[k, h] = res
                if k:
                    go(remote(
                        r_send.at[k, h], r_got.at[k, h], r_ssem.at[k, h], r_rsem.at[k, h], dev(n_y - k, 0, 0)
                    ))
            send_m(M_STEPS[2])
    send_m(len(left))
    for h in range(2):
        finish(h, r_send[0, h], y)
        for k in order_y:
            wait_in(r_got.at[k, h], r_rsem.at[k, h])
            finish(h, r_got[k, h], ys[k])

    for copy in m_copies:
        copy.wait_recv()
    keep.wait()
    for s in range(seq_own):
        msa_ref[s] = m_got[:, s].astype(F32).reshape(n_res, chans).astype(BF16)
    for copy in sends:
        copy.wait_send()


def store(pair_v, msa_v, pair_ref, msa_ref, sem):
    copies = [pltpu.make_async_copy(pair_v, pair_ref, sem.at[0]), pltpu.make_async_copy(msa_v, msa_ref, sem.at[1])]
    for copy in copies:
        copy.start()
    for copy in copies:
        copy.wait()


def solution(mesh):
    n_y, n_dap = mesh.shape["outer"], mesh.shape["dap"]
    n_x, n_dev = n_dap // 2, n_y * n_dap
    dap_axes = ("outer", "dap")
    group_axes = ("data", "outer", "dap")

    def local_step(msa, mask, pair, gamma, beta, w_left, b_left, w_right, b_right, w_out, b_out):
        n_seq, rows, chans = msa.shape
        n_res = mask.shape[1]
        opm = w_left.shape[1]
        pair_dim = w_out.shape[1]
        seq_own = n_seq // n_dev
        line = n_x * rows
        dma = pltpu.SemaphoreType.DMA
        vmem = pl.BlockSpec(memory_space=pltpu.VMEM)
        ins = (msa, mask, pair, gamma, beta, w_left.T, b_left, w_right.T, b_right, w_out, b_out)
        got = pl.pallas_call(
            functools.partial(kernel, n_y, n_dap),
            out_shape=(
                pltpu.VMEM(pair.shape, F32),
                pltpu.VMEM((seq_own, n_dev * rows, chans), BF16),
            ),
            in_specs=[pl.BlockSpec(memory_space=pl.ANY)] * len(ins),
            out_specs=(vmem, vmem),
            scratch_shapes=[pltpu.VMEM(v.shape, v.dtype) for v in ins[:2] + ins[3:]] + [
                pltpu.VMEM((n_dev, seq_own, rows, chans), BF16),
                pltpu.VMEM((n_seq * rows, 2 * opm), F32),
                pltpu.VMEM((n_y, n_seq, rows * opm), BF16),
                pltpu.VMEM((n_dap, rows * opm, n_seq), BF16),
                pltpu.VMEM((2, line * opm, rows * opm), F32),
                pltpu.VMEM((opm * opm, pair_dim), F32),
                pltpu.VMEM((opm * opm, pair_dim), BF16),
                pltpu.VMEM((2 * rows * line, opm * opm), BF16),
                pltpu.VMEM((rows, n_res, pair_dim), F32),
                pltpu.VMEM((n_y, 2, rows * line, pair_dim), F32),
                pltpu.VMEM((n_y, 2, rows * line, pair_dim), F32),
                dma((10,)), dma((LN_CHUNKS,)), dma, dma((n_dev - 1,)), dma((n_dev - 1,)),
                dma((n_y,)), dma((n_y,)), dma((n_x,)), dma((n_x,)), dma((n_x,)), dma((n_x,)), dma((n_y, 2)), dma((n_y, 2)),
            ],
            compiler_params=pltpu.CompilerParams(collective_id=0, has_side_effects=True),
        )(*ins)
        return pl.pallas_call(
            store,
            out_shape=tuple(jax.ShapeDtypeStruct(v.shape, v.dtype) for v in got),
            in_specs=[pl.BlockSpec(memory_space=pl.ANY)] * 2,
            out_specs=(pl.BlockSpec(memory_space=pl.ANY),) * 2,
            scratch_shapes=[dma((2,))],
            compiler_params=pltpu.CompilerParams(vmem_limit_bytes=4 * 1024 * 1024),
        )(*got)

    return jax.shard_map(
        local_step, mesh=mesh,
        in_specs=(P("data", dap_axes, None), P("data", None), P(group_axes, None, None)) + (P(),) * 8,
        out_specs=(P(group_axes, None, None), P(group_axes, None, None)), check_vma=False,
    )
```

```python
import functools

import jax
import jax.numpy as jnp
from jax import lax
from jax.experimental import pallas as pl
from jax.experimental.pallas import tpu as pltpu
from jax.sharding import PartitionSpec as P

LN_EPS = 1e-5
NORM_EPS = 1e-3
MESH = pl.DeviceIdType.MESH
F32 = jnp.float32
BF16 = jnp.bfloat16
LN_CHUNKS = 1

M_FIRST = 0
M_STEPS = (31, 0, 0)


def kernel(
    n_y, n_dap,
    m_hbm, mask_hbm, z_hbm, gamma_hbm, beta_hbm, wl_hbm, bl_hbm, wr_hbm, br_hbm, wo_hbm, bo_hbm,
    pair_ref, msa_ref,
    m_v, mask_v, gamma_v, beta_v, wl_v, bl_v, wr_v, br_v, wo_v, bo_v,
    m_got, y_s, a_all, b_row, o_s, w_s, w_perm, lhs_s, den_s, r_send, r_got,
    in_sem, m_sem, own_sem, m_send, m_recv,
    a_send, a_recv, b_send, b_recv, p_send, p_recv, r_ssem, r_rsem,
):
    n_x = n_dap // 2
    n_dev = n_y * n_dap
    n_seq, rows, chans = m_v.shape
    seq_own = n_seq // n_dev
    opm = wl_v.shape[0]
    n_res = mask_v.shape[1]
    line = n_x * rows
    y = lax.axis_index("outer")
    d = lax.axis_index("dap")
    x, c = d // 2, d % 2
    me = y * n_dap + d

    ys = [lax.rem(y + k, n_y) for k in range(n_y)]
    xs = [lax.rem(x + k, n_x) for k in range(n_x)]
    cs = [c, 1 - c]

    def dev(dy, dx, dc):
        return {"outer": ys[dy % n_y], "dap": xs[dx % n_x] * 2 + cs[dc]}

    def remote(src, dst, send, recv, where):
        return pltpu.make_async_remote_copy(
            src_ref=src, dst_ref=dst, send_sem=send, recv_sem=recv, device_id=where, device_id_type=MESH
        )

    def wait_in(ref, sem):
        remote(ref, ref, sem, sem, dev(0, 0, 1)).wait_recv()

    order_x = list(range(2, n_x - 1)) + [1, n_x - 1]
    order_y = list(range(2, n_y - 1)) + [1, n_y - 1]
    offsets = [(dy, dx, dc) for dx in range(n_x) for dy in range(n_y) for dc in range(2) if dy or dx or dc]

    offsets.sort(key=lambda o: (-o[2], -(min(o[0], n_y - o[0]) + min(o[1], n_x - o[1]))))

    piece = n_seq // LN_CHUNKS
    m_in = []
    for k in range(LN_CHUNKS):
        part = pl.ds(k * piece, piece)
        m_in.append(pltpu.make_async_copy(m_hbm.at[part], m_v.at[part], m_sem.at[k]))
    pairs = [
        (gamma_hbm, gamma_v), (beta_hbm, beta_v), (wl_hbm, wl_v), (wr_hbm, wr_v), (bl_hbm, bl_v), (br_hbm, br_v),
        (mask_hbm, mask_v), (wo_hbm, wo_v), (bo_hbm, bo_v), (z_hbm, pair_ref),
    ]
    small_in = [pltpu.make_async_copy(src, dst, in_sem.at[i]) for i, (src, dst) in enumerate(pairs)]
    for copy in small_in[6:7] + m_in + small_in[:6] + small_in[7:]:
        copy.start()
    barrier = pltpu.get_barrier_semaphore()
    for off in offsets:
        pl.semaphore_signal(barrier, inc=1, device_id=dev(*off), device_id_type=MESH)

    m_copies = []
    for i, off in enumerate(offsets):
        to = dev(*off)
        p = to["outer"] * n_dap + to["dap"]
        m_copies.append(
            remote(m_v.at[pl.ds(p * seq_own, seq_own)], m_got.at[me], m_send, m_recv, to)
        )

    small_in[6].wait()
    mask_b = mask_v[...].astype(F32).astype(BF16)
    row_of = lax.broadcasted_iota(jnp.int32, (n_res, rows * opm), 0)
    col_of = lax.broadcasted_iota(jnp.int32, (n_res, rows * opm), 1)
    pick = jnp.where(row_of == me * rows + col_of // opm, 1.0, 0.0).astype(BF16)
    mask_own = jnp.dot(mask_b, pick, preferred_element_type=F32)

    for copy in small_in[:6]:
        copy.wait()
    w_both = jnp.concatenate([wl_v[...], wr_v[...]], axis=0)
    b_both = jnp.concatenate([bl_v[...].astype(F32), br_v[...].astype(F32)]).reshape(1, 2 * opm)
    gamma = gamma_v[...].astype(F32).reshape(1, chans)
    beta = beta_v[...].astype(F32).reshape(1, chans)

    def normalise(k):
        m_in[k].wait()
        v = m_v[k * piece:(k + 1) * piece].astype(F32).reshape(piece * rows, chans)
        mean = jnp.mean(v, axis=-1, keepdims=True)
        cen = v - mean
        var = jnp.mean(cen * cen, axis=-1, keepdims=True)
        xn = (cen * lax.rsqrt(var + LN_EPS) * gamma + beta).astype(BF16)
        out = lax.dot_general(xn, w_both, (((1,), (1,)), ((), ())), preferred_element_type=F32) + b_both
        y_s[k * piece * rows:(k + 1) * piece * rows, :] = out

    for k in range(LN_CHUNKS):
        normalise(k)

    proj = [y_s[pl.ds(r, n_seq, stride=rows), :] for r in range(rows)]
    a_all[0] = (jnp.concatenate([t[:, :opm] for t in proj], axis=1) * mask_own).astype(BF16)
    b_own = jnp.concatenate([t[:, opm:] for t in proj], axis=1) * mask_own
    b_row[x] = b_own.T.astype(BF16)

    left = list(m_copies)

    def send_m(count):
        for _ in range(min(count, len(left))):
            left.pop(0).start()

    pl.semaphore_wait(barrier, n_dev - 1)
    send_m(M_FIRST)
    mine = b_row.at[x]
    remote(mine, b_row.at[n_x + x], p_send, p_recv.at[0], dev(0, 0, 1)).start()
    for kx, ky in zip(order_x, order_y, strict=True):
        remote(mine, mine, b_send, b_recv.at[kx], dev(0, kx, 0)).start()
        remote(a_all.at[0], a_all.at[ky], a_send, a_recv.at[ky], dev(ky, 0, 0)).start()
    keep = pltpu.make_async_copy(m_v.at[pl.ds(me * seq_own, seq_own)], m_got.at[me], own_sem)
    keep.start()
    send_m(M_STEPS[0])

    for copy in small_in[7:]:
        copy.wait()
    w_s[...] = wo_v[...].astype(F32)
    for e in range(opm):
        w_perm[e * opm:(e + 1) * opm, :] = w_s[pl.ds(e, opm, stride=opm), :].astype(BF16)
    count = lax.dot_general(
        mask_b, mask_own.astype(BF16), (((0,), (0,)), ((), ())), preferred_element_type=F32
    )
    for i in range(rows):
        den_s[i] = jnp.broadcast_to(NORM_EPS + count[:, i * opm:i * opm + 1], den_s.shape[1:])
    bias_out = bo_v[...].astype(F32).reshape(1, -1)

    for k in order_x:
        at = xs[n_x - k]
        got = b_row.at[at]
        wait_in(got, b_recv.at[k])
        remote(got, b_row.at[n_x + at], p_send, p_recv.at[0], dev(0, 0, 1)).start()
    send_m(M_STEPS[1])

    per = 128 // opm

    def outer(h, slots):
        b_line = b_row[h * n_x:(h + 1) * n_x].reshape(line * opm, n_seq)
        a_pair = jnp.concatenate([a_all[k] for k in slots], axis=1)
        both = jnp.dot(b_line, a_pair, preferred_element_type=F32)
        for t in range(len(slots)):
            o_s[t] = both[:, t * rows * opm:(t + 1) * rows * opm]
        for g in range(opm // per):
            for t in range(len(slots)):
                parts = [o_s[t, pl.ds(g * per + q, line, stride=opm), :].astype(BF16) for q in range(per)]
                for i in range(rows):
                    block = jnp.concatenate([v[:, i * opm:(i + 1) * opm] for v in parts], axis=1)
                    to = (t * rows + i) * line
                    lhs_s[to:to + line, g * 128:(g + 1) * 128] = block.astype(BF16)
        res = jnp.dot(lhs_s[:len(slots) * rows * line], w_perm[...], preferred_element_type=F32)
        return [res[t * rows * line:(t + 1) * rows * line] for t in range(len(slots))]

    def finish(h, res, row):
        for i in range(rows):
            for t in range(n_x):
                at = pl.ds((row * n_x + t) * 2 * rows + cs[h] * rows, rows)
                part = res[(i * n_x + t) * rows:(i * n_x + t + 1) * rows]
                pair_ref[i, at, :] += (part + bias_out) / den_s[i, at, :]

    for h in range(2):
        if h == 1:
            wait_in(b_row.at[pl.ds(n_x, n_x)], p_recv.at[0])
        for slots in (order_y[:1], order_y[1:]):
            if h == 0:
                for k in slots:
                    wait_in(a_all.at[k], a_recv.at[k])
            for k, res in zip(slots, outer(h, slots), strict=True):
                r_send[k, h] = res
                remote(r_send.at[k, h], r_got.at[k, h], r_ssem, r_rsem.at[k, h], dev(n_y - k, 0, 0)).start()
    send_m(len(left))
    for h in range(2):
        finish(h, outer(h, [0])[0], y)
    for h in range(2):
        for k in order_y:
            wait_in(r_got.at[k, h], r_rsem.at[k, h])
            finish(h, r_got[k, h], ys[k])

    arrived = m_got.at[pl.ds(0, n_dev - 1)]
    wait_in(arrived, m_recv)
    keep.wait()
    for s in range(seq_own):
        msa_ref[s] = m_got[:, s].astype(F32).reshape(n_res, chans).astype(BF16)
    for ref, sem in [
        (arrived, m_send), (a_all.at[pl.ds(0, n_y - 1)], a_send), (b_row.at[pl.ds(0, n_x - 1)], b_send),
        (b_row.at[pl.ds(0, n_x)], p_send), (r_send.at[pl.ds(0, n_y - 1)], r_ssem),
    ]:
        remote(ref, ref, sem, sem, dev(0, 0, 1)).wait_send()


def store(pair_v, msa_v, pair_ref, msa_ref, sem):
    copies = [pltpu.make_async_copy(pair_v, pair_ref, sem.at[0]), pltpu.make_async_copy(msa_v, msa_ref, sem.at[1])]
    for copy in copies:
        copy.start()
    for copy in copies:
        copy.wait()


def solution(mesh):
    n_y, n_dap = mesh.shape["outer"], mesh.shape["dap"]
    n_x, n_dev = n_dap // 2, n_y * n_dap
    dap_axes = ("outer", "dap")
    group_axes = ("data", "outer", "dap")

    def local_step(msa, mask, pair, gamma, beta, w_left, b_left, w_right, b_right, w_out, b_out):
        n_seq, rows, chans = msa.shape
        n_res = mask.shape[1]
        opm = w_left.shape[1]
        pair_dim = w_out.shape[1]
        seq_own = n_seq // n_dev
        line = n_x * rows
        dma = pltpu.SemaphoreType.DMA
        vmem = pl.BlockSpec(memory_space=pltpu.VMEM)
        ins = (msa, mask, pair, gamma, beta, w_left.T, b_left, w_right.T, b_right, w_out, b_out)
        got = pl.pallas_call(
            functools.partial(kernel, n_y, n_dap),
            out_shape=(
                pltpu.VMEM(pair.shape, F32),
                pltpu.VMEM((seq_own, n_dev * rows, chans), BF16),
            ),
            in_specs=[pl.BlockSpec(memory_space=pl.ANY)] * len(ins),
            out_specs=(vmem, vmem),
            scratch_shapes=[pltpu.VMEM(v.shape, v.dtype) for v in ins[:2] + ins[3:]] + [
                pltpu.VMEM((n_dev, seq_own, rows, chans), BF16),
                pltpu.VMEM((n_seq * rows, 2 * opm), F32),
                pltpu.VMEM((n_y, n_seq, rows * opm), BF16),
                pltpu.VMEM((n_dap, rows * opm, n_seq), BF16),
                pltpu.VMEM((2, line * opm, rows * opm), F32),
                pltpu.VMEM((opm * opm, pair_dim), F32),
                pltpu.VMEM((opm * opm, pair_dim), BF16),
                pltpu.VMEM((2 * rows * line, opm * opm), BF16),
                pltpu.VMEM((rows, n_res, pair_dim), F32),
                pltpu.VMEM((n_y, 2, rows * line, pair_dim), F32),
                pltpu.VMEM((n_y, 2, rows * line, pair_dim), F32),
                dma((10,)), dma((LN_CHUNKS,)), dma, dma, dma,
                dma, dma((n_y,)), dma, dma((n_x,)), dma, dma((1,)), dma, dma((n_y, 2)),
            ],
            compiler_params=pltpu.CompilerParams(collective_id=0, has_side_effects=True),
        )(*ins)
        return pl.pallas_call(
            store,
            out_shape=tuple(jax.ShapeDtypeStruct(v.shape, v.dtype) for v in got),
            in_specs=[pl.BlockSpec(memory_space=pl.ANY)] * 2,
            out_specs=(pl.BlockSpec(memory_space=pl.ANY),) * 2,
            scratch_shapes=[dma((2,))],
            compiler_params=pltpu.CompilerParams(vmem_limit_bytes=4 * 1024 * 1024),
        )(*got)

    return jax.shard_map(
        local_step, mesh=mesh,
        in_specs=(P("data", dap_axes, None), P("data", None), P(group_axes, None, None)) + (P(),) * 8,
        out_specs=(P(group_axes, None, None), P(group_axes, None, None)), check_vma=False,
    )
```

```python
import functools

import jax
import jax.numpy as jnp
from jax import lax
from jax.experimental import pallas as pl
from jax.experimental.pallas import tpu as pltpu
from jax.sharding import PartitionSpec as P

LN_EPS = 1e-5
NORM_EPS = 1e-3
MESH = pl.DeviceIdType.MESH
F32 = jnp.float32
BF16 = jnp.bfloat16
LN_CHUNKS = 1

M_FIRST = 0
M_STEPS = (31, 0, 0)


def kernel(
    n_y, n_dap,
    m_hbm, mask_hbm, z_hbm, gamma_hbm, beta_hbm, wl_hbm, bl_hbm, wr_hbm, br_hbm, wo_hbm, bo_hbm,
    pair_ref, msa_ref,
    m_v, mask_v, gamma_v, beta_v, wl_v, bl_v, wr_v, br_v, wo_v, bo_v,
    m_got, y_s, a_all, b_row, o_s, w_s, w_perm, lhs_s, den_s, r_send, r_got,
    in_sem, m_sem, own_sem, m_send, m_recv,
    a_send, a_recv, b_send, b_recv, p_send, p_recv, r_ssem, r_rsem,
):
    n_x = n_dap // 2
    n_dev = n_y * n_dap
    n_seq, rows, chans = m_v.shape
    seq_own = n_seq // n_dev
    opm = wl_v.shape[0]
    n_res = mask_v.shape[1]
    line = n_x * rows
    y = lax.axis_index("outer")
    d = lax.axis_index("dap")
    x, c = d // 2, d % 2
    me = y * n_dap + d

    ys = [lax.rem(y + k, n_y) for k in range(n_y)]
    xs = [lax.rem(x + k, n_x) for k in range(n_x)]
    cs = [c, 1 - c]

    def dev(dy, dx, dc):
        return {"outer": ys[dy % n_y], "dap": xs[dx % n_x] * 2 + cs[dc]}

    def remote(src, dst, send, recv, where):
        return pltpu.make_async_remote_copy(
            src_ref=src, dst_ref=dst, send_sem=send, recv_sem=recv, device_id=where, device_id_type=MESH
        )

    def wait_in(ref, sem):
        remote(ref, ref, sem, sem, dev(0, 0, 1)).wait_recv()

    order_x = list(range(2, n_x - 1)) + [1, n_x - 1]
    order_y = list(range(2, n_y - 1)) + [1, n_y - 1]
    offsets = [(dy, dx, dc) for dx in range(n_x) for dy in range(n_y) for dc in range(2) if dy or dx or dc]

    offsets.sort(key=lambda o: (-o[2], -(min(o[0], n_y - o[0]) + min(o[1], n_x - o[1]))))

    piece = n_seq // LN_CHUNKS
    m_in = []
    for k in range(LN_CHUNKS):
        part = pl.ds(k * piece, piece)
        m_in.append(pltpu.make_async_copy(m_hbm.at[part], m_v.at[part], m_sem.at[k]))
    pairs = [
        (gamma_hbm, gamma_v), (beta_hbm, beta_v), (wl_hbm, wl_v), (wr_hbm, wr_v), (bl_hbm, bl_v), (br_hbm, br_v),
        (mask_hbm, mask_v), (wo_hbm, wo_v), (bo_hbm, bo_v), (z_hbm, pair_ref),
    ]
    small_in = [pltpu.make_async_copy(src, dst, in_sem.at[i]) for i, (src, dst) in enumerate(pairs)]
    for copy in small_in[6:7] + m_in + small_in[:6] + small_in[7:]:
        copy.start()
    barrier = pltpu.get_barrier_semaphore()
    for off in offsets:
        pl.semaphore_signal(barrier, inc=1, device_id=dev(*off), device_id_type=MESH)

    m_copies = []
    for i, off in enumerate(offsets):
        to = dev(*off)
        p = to["outer"] * n_dap + to["dap"]
        m_copies.append(
            remote(m_v.at[pl.ds(p * seq_own, seq_own)], m_got.at[me], m_send, m_recv, to)
        )

    small_in[6].wait()
    mask_b = mask_v[...].astype(F32).astype(BF16)
    row_of = lax.broadcasted_iota(jnp.int32, (n_res, rows * opm), 0)
    col_of = lax.broadcasted_iota(jnp.int32, (n_res, rows * opm), 1)
    pick = jnp.where(row_of == me * rows + col_of // opm, 1.0, 0.0).astype(BF16)
    mask_own = jnp.dot(mask_b, pick, preferred_element_type=F32)

    for copy in small_in[:6]:
        copy.wait()
    w_both = jnp.concatenate([wl_v[...], wr_v[...]], axis=0)
    b_both = jnp.concatenate([bl_v[...].astype(F32), br_v[...].astype(F32)]).reshape(1, 2 * opm)
    gamma = gamma_v[...].astype(F32).reshape(1, chans)
    beta = beta_v[...].astype(F32).reshape(1, chans)

    def normalise(k):
        m_in[k].wait()
        v = m_v[k * piece:(k + 1) * piece].astype(F32).reshape(piece * rows, chans)
        mean = jnp.mean(v, axis=-1, keepdims=True)
        cen = v - mean
        var = jnp.mean(cen * cen, axis=-1, keepdims=True)
        xn = (cen * lax.rsqrt(var + LN_EPS) * gamma + beta).astype(BF16)
        out = lax.dot_general(xn, w_both, (((1,), (1,)), ((), ())), preferred_element_type=F32) + b_both
        y_s[k * piece * rows:(k + 1) * piece * rows, :] = out

    for k in range(LN_CHUNKS):
        normalise(k)

    proj = [y_s[pl.ds(r, n_seq, stride=rows), :] for r in range(rows)]
    a_all[0] = (jnp.concatenate([t[:, :opm] for t in proj], axis=1) * mask_own).astype(BF16)
    b_own = jnp.concatenate([t[:, opm:] for t in proj], axis=1) * mask_own
    b_row[x] = b_own.T.astype(BF16)

    left = list(m_copies)

    def send_m(count):
        for _ in range(min(count, len(left))):
            left.pop(0).start()

    pl.semaphore_wait(barrier, n_dev - 1)
    send_m(M_FIRST)
    mine = b_row.at[x]
    for kx, ky in zip(order_x, order_y, strict=True):
        remote(mine, mine, b_send, b_recv.at[kx], dev(0, kx, 0)).start()
        remote(a_all.at[0], a_all.at[ky], a_send, a_recv.at[ky], dev(ky, 0, 0)).start()
    remote(mine, b_row.at[n_x + x], p_send, p_recv.at[0], dev(0, 0, 1)).start()
    keep = pltpu.make_async_copy(m_v.at[pl.ds(me * seq_own, seq_own)], m_got.at[me], own_sem)
    keep.start()
    send_m(M_STEPS[0])

    for copy in small_in[7:]:
        copy.wait()
    w_s[...] = wo_v[...].astype(F32)
    for e in range(opm):
        w_perm[e * opm:(e + 1) * opm, :] = w_s[pl.ds(e, opm, stride=opm), :].astype(BF16)
    count = lax.dot_general(
        mask_b, mask_own.astype(BF16), (((0,), (0,)), ((), ())), preferred_element_type=F32
    )
    for i in range(rows):
        den_s[i] = jnp.broadcast_to(NORM_EPS + count[:, i * opm:i * opm + 1], den_s.shape[1:])
    bias_out = bo_v[...].astype(F32).reshape(1, -1)

    for k in order_x:
        at = xs[n_x - k]
        got = b_row.at[at]
        wait_in(got, b_recv.at[k])
        remote(got, b_row.at[n_x + at], p_send, p_recv.at[0], dev(0, 0, 1)).start()
    send_m(M_STEPS[1])

    per = 128 // opm

    def outer(h, slots):
        b_line = b_row[h * n_x:(h + 1) * n_x].reshape(line * opm, n_seq)
        a_pair = jnp.concatenate([a_all[k] for k in slots], axis=1)
        both = jnp.dot(b_line, a_pair, preferred_element_type=F32)
        for t in range(len(slots)):
            o_s[t] = both[:, t * rows * opm:(t + 1) * rows * opm]
        for g in range(opm // per):
            for t in range(len(slots)):
                parts = [o_s[t, pl.ds(g * per + q, line, stride=opm), :].astype(BF16) for q in range(per)]
                for i in range(rows):
                    block = jnp.concatenate([v[:, i * opm:(i + 1) * opm] for v in parts], axis=1)
                    to = (t * rows + i) * line
                    lhs_s[to:to + line, g * 128:(g + 1) * 128] = block.astype(BF16)
        res = jnp.dot(lhs_s[:len(slots) * rows * line], w_perm[...], preferred_element_type=F32)
        return [res[t * rows * line:(t + 1) * rows * line] for t in range(len(slots))]

    def finish(h, res, row):
        for i in range(rows):
            for t in range(n_x):
                at = pl.ds((row * n_x + t) * 2 * rows + cs[h] * rows, rows)
                part = res[(i * n_x + t) * rows:(i * n_x + t + 1) * rows]
                pair_ref[i, at, :] += (part + bias_out) / den_s[i, at, :]

    for h in range(2):
        if h == 1:
            wait_in(b_row.at[pl.ds(n_x, n_x)], p_recv.at[0])
        for slots in (order_y[:1], order_y[1:]):
            if h == 0:
                for k in slots:
                    wait_in(a_all.at[k], a_recv.at[k])
            for k, res in zip(slots, outer(h, slots), strict=True):
                r_send[k, h] = res
                remote(r_send.at[k, h], r_got.at[k, h], r_ssem, r_rsem.at[k, h], dev(n_y - k, 0, 0)).start()
    send_m(len(left))
    for h in range(2):
        finish(h, outer(h, [0])[0], y)
    arrived = m_got.at[pl.ds(0, n_dev - 1)]
    wait_in(arrived, m_recv)
    keep.wait()
    for s in range(seq_own):
        msa_ref[s] = m_got[:, s].astype(F32).reshape(n_res, chans).astype(BF16)
    for h in range(2):
        for k in order_y:
            wait_in(r_got.at[k, h], r_rsem.at[k, h])
            finish(h, r_got[k, h], ys[k])

    for ref, sem in [
        (arrived, m_send), (a_all.at[pl.ds(0, n_y - 1)], a_send), (b_row.at[pl.ds(0, n_x - 1)], b_send),
        (b_row.at[pl.ds(0, n_x)], p_send), (r_send.at[pl.ds(0, n_y - 1)], r_ssem),
    ]:
        remote(ref, ref, sem, sem, dev(0, 0, 1)).wait_send()


def store(pair_v, msa_v, pair_ref, msa_ref, sem):
    copies = [pltpu.make_async_copy(pair_v, pair_ref, sem.at[0]), pltpu.make_async_copy(msa_v, msa_ref, sem.at[1])]
    for copy in copies:
        copy.start()
    for copy in copies:
        copy.wait()


def solution(mesh):
    n_y, n_dap = mesh.shape["outer"], mesh.shape["dap"]
    n_x, n_dev = n_dap // 2, n_y * n_dap
    dap_axes = ("outer", "dap")
    group_axes = ("data", "outer", "dap")

    def local_step(msa, mask, pair, gamma, beta, w_left, b_left, w_right, b_right, w_out, b_out):
        n_seq, rows, chans = msa.shape
        n_res = mask.shape[1]
        opm = w_left.shape[1]
        pair_dim = w_out.shape[1]
        seq_own = n_seq // n_dev
        line = n_x * rows
        dma = pltpu.SemaphoreType.DMA
        vmem = pl.BlockSpec(memory_space=pltpu.VMEM)
        ins = (msa, mask, pair, gamma, beta, w_left.T, b_left, w_right.T, b_right, w_out, b_out)
        got = pl.pallas_call(
            functools.partial(kernel, n_y, n_dap),
            out_shape=(
                pltpu.VMEM(pair.shape, F32),
                pltpu.VMEM((seq_own, n_dev * rows, chans), BF16),
            ),
            in_specs=[pl.BlockSpec(memory_space=pl.ANY)] * len(ins),
            out_specs=(vmem, vmem),
            scratch_shapes=[pltpu.VMEM(v.shape, v.dtype) for v in ins[:2] + ins[3:]] + [
                pltpu.VMEM((n_dev, seq_own, rows, chans), BF16),
                pltpu.VMEM((n_seq * rows, 2 * opm), F32),
                pltpu.VMEM((n_y, n_seq, rows * opm), BF16),
                pltpu.VMEM((n_dap, rows * opm, n_seq), BF16),
                pltpu.VMEM((2, line * opm, rows * opm), F32),
                pltpu.VMEM((opm * opm, pair_dim), F32),
                pltpu.VMEM((opm * opm, pair_dim), BF16),
                pltpu.VMEM((2 * rows * line, opm * opm), BF16),
                pltpu.VMEM((rows, n_res, pair_dim), F32),
                pltpu.VMEM((n_y, 2, rows * line, pair_dim), F32),
                pltpu.VMEM((n_y, 2, rows * line, pair_dim), F32),
                dma((10,)), dma((LN_CHUNKS,)), dma, dma, dma,
                dma, dma((n_y,)), dma, dma((n_x,)), dma, dma((1,)), dma, dma((n_y, 2)),
            ],
            compiler_params=pltpu.CompilerParams(collective_id=0, has_side_effects=True),
        )(*ins)
        return pl.pallas_call(
            store,
            out_shape=tuple(jax.ShapeDtypeStruct(v.shape, v.dtype) for v in got),
            in_specs=[pl.BlockSpec(memory_space=pl.ANY)] * 2,
            out_specs=(pl.BlockSpec(memory_space=pl.ANY),) * 2,
            scratch_shapes=[dma((2,))],
            compiler_params=pltpu.CompilerParams(vmem_limit_bytes=4 * 1024 * 1024),
        )(*got)

    return jax.shard_map(
        local_step, mesh=mesh,
        in_specs=(P("data", dap_axes, None), P("data", None), P(group_axes, None, None)) + (P(),) * 8,
        out_specs=(P(group_axes, None, None), P(group_axes, None, None)), check_vma=False,
    )
```

```python
import functools

import jax
import jax.numpy as jnp
from jax import lax
from jax.experimental import pallas as pl
from jax.experimental.pallas import tpu as pltpu
from jax.sharding import PartitionSpec as P

LN_EPS = 1e-5
NORM_EPS = 1e-3
MESH = pl.DeviceIdType.MESH
F32 = jnp.float32
BF16 = jnp.bfloat16
LN_CHUNKS = 1

M_FIRST = 0
M_STEPS = (31, 0, 0)


def kernel(
    n_y, n_dap,
    m_hbm, mask_hbm, z_hbm, gamma_hbm, beta_hbm, wl_hbm, bl_hbm, wr_hbm, br_hbm, wo_hbm, bo_hbm,
    pair_ref, msa_ref,
    m_v, mask_v, gamma_v, beta_v, wl_v, bl_v, wr_v, br_v, wo_v, bo_v,
    m_got, y_s, a_all, b_row, o_s, w_s, w_perm, lhs_s, den_s, r_send, r_got,
    in_sem, m_sem, own_sem, m_send, m_recv,
    a_send, a_recv, b_send, b_recv, p_send, p_recv, r_ssem, r_rsem,
):
    n_x = n_dap // 2
    n_dev = n_y * n_dap
    n_seq, rows, chans = m_v.shape
    seq_own = n_seq // n_dev
    opm = wl_v.shape[0]
    n_res = mask_v.shape[1]
    line = n_x * rows
    y = lax.axis_index("outer")
    d = lax.axis_index("dap")
    x, c = d // 2, d % 2
    me = y * n_dap + d

    ys = [lax.rem(y + k, n_y) for k in range(n_y)]
    xs = [lax.rem(x + k, n_x) for k in range(n_x)]
    cs = [c, 1 - c]

    def dev(dy, dx, dc):
        return {"outer": ys[dy % n_y], "dap": xs[dx % n_x] * 2 + cs[dc]}

    def remote(src, dst, send, recv, where):
        return pltpu.make_async_remote_copy(
            src_ref=src, dst_ref=dst, send_sem=send, recv_sem=recv, device_id=where, device_id_type=MESH
        )

    def wait_in(ref, sem):
        remote(ref, ref, sem, sem, dev(0, 0, 1)).wait_recv()

    order_x = list(range(2, n_x - 1)) + [1, n_x - 1]
    order_y = list(range(2, n_y - 1)) + [1, n_y - 1]
    offsets = [(dy, dx, dc) for dx in range(n_x) for dy in range(n_y) for dc in range(2) if dy or dx or dc]

    offsets.sort(key=lambda o: (-o[2], -(min(o[0], n_y - o[0]) + min(o[1], n_x - o[1]))))

    piece = n_seq // LN_CHUNKS
    m_in = []
    for k in range(LN_CHUNKS):
        part = pl.ds(k * piece, piece)
        m_in.append(pltpu.make_async_copy(m_hbm.at[part], m_v.at[part], m_sem.at[k]))
    pairs = [
        (gamma_hbm, gamma_v), (beta_hbm, beta_v), (wl_hbm, wl_v), (wr_hbm, wr_v), (bl_hbm, bl_v), (br_hbm, br_v),
        (mask_hbm, mask_v), (wo_hbm, wo_v), (bo_hbm, bo_v), (z_hbm, pair_ref),
    ]
    small_in = [pltpu.make_async_copy(src, dst, in_sem.at[i]) for i, (src, dst) in enumerate(pairs)]
    for copy in small_in[6:7] + m_in + small_in[:6] + small_in[7:]:
        copy.start()
    barrier = pltpu.get_barrier_semaphore()
    for off in offsets:
        pl.semaphore_signal(barrier, inc=1, device_id=dev(*off), device_id_type=MESH)

    m_copies = []
    for i, off in enumerate(offsets):
        to = dev(*off)
        p = to["outer"] * n_dap + to["dap"]
        m_copies.append(
            remote(m_v.at[pl.ds(p * seq_own, seq_own)], m_got.at[me], m_send, m_recv, to)
        )

    small_in[6].wait()
    mask_b = mask_v[...].astype(F32).astype(BF16)
    row_of = lax.broadcasted_iota(jnp.int32, (n_res, rows * opm), 0)
    col_of = lax.broadcasted_iota(jnp.int32, (n_res, rows * opm), 1)
    pick = jnp.where(row_of == me * rows + col_of // opm, 1.0, 0.0).astype(BF16)
    mask_own = jnp.dot(mask_b, pick, preferred_element_type=F32)

    for copy in small_in[:6]:
        copy.wait()
    w_both = jnp.concatenate([wl_v[...], wr_v[...]], axis=0)
    b_both = jnp.concatenate([bl_v[...].astype(F32), br_v[...].astype(F32)]).reshape(1, 2 * opm)
    gamma = gamma_v[...].astype(F32).reshape(1, chans)
    beta = beta_v[...].astype(F32).reshape(1, chans)

    def normalise(k):
        m_in[k].wait()
        v = m_v[k * piece:(k + 1) * piece].astype(F32).reshape(piece * rows, chans)
        mean = jnp.mean(v, axis=-1, keepdims=True)
        cen = v - mean
        var = jnp.mean(cen * cen, axis=-1, keepdims=True)
        xn = (cen * lax.rsqrt(var + LN_EPS) * gamma + beta).astype(BF16)
        out = lax.dot_general(xn, w_both, (((1,), (1,)), ((), ())), preferred_element_type=F32) + b_both
        y_s[k * piece * rows:(k + 1) * piece * rows, :] = out

    for k in range(LN_CHUNKS):
        normalise(k)

    proj = [y_s[pl.ds(r, n_seq, stride=rows), :] for r in range(rows)]
    a_all[0] = (jnp.concatenate([t[:, :opm] for t in proj], axis=1) * mask_own).astype(BF16)
    b_own = jnp.concatenate([t[:, opm:] for t in proj], axis=1) * mask_own
    b_row[x] = b_own.T.astype(BF16)

    left = list(m_copies)

    def send_m(count):
        for _ in range(min(count, len(left))):
            left.pop(0).start()

    pl.semaphore_wait(barrier, n_dev - 1)
    send_m(M_FIRST)
    mine = b_row.at[x]
    for kx, ky in zip(order_x, order_y, strict=True):
        remote(mine, mine, b_send, b_recv.at[kx], dev(0, kx, 0)).start()
        remote(a_all.at[0], a_all.at[ky], a_send, a_recv.at[ky], dev(ky, 0, 0)).start()
    remote(mine, b_row.at[n_x + x], p_send, p_recv.at[0], dev(0, 0, 1)).start()
    keep = pltpu.make_async_copy(m_v.at[pl.ds(me * seq_own, seq_own)], m_got.at[me], own_sem)
    keep.start()
    send_m(M_STEPS[0])

    for copy in small_in[7:]:
        copy.wait()
    w_s[...] = wo_v[...].astype(F32)
    for e in range(opm):
        w_perm[e * opm:(e + 1) * opm, :] = w_s[pl.ds(e, opm, stride=opm), :].astype(BF16)
    count = lax.dot_general(
        mask_b, mask_own.astype(BF16), (((0,), (0,)), ((), ())), preferred_element_type=F32
    )
    for i in range(rows):
        den_s[i] = 1.0 / jnp.broadcast_to(NORM_EPS + count[:, i * opm:i * opm + 1], den_s.shape[1:])
    bias_out = bo_v[...].astype(F32).reshape(1, -1)

    for k in order_x:
        at = xs[n_x - k]
        got = b_row.at[at]
        wait_in(got, b_recv.at[k])
        remote(got, b_row.at[n_x + at], p_send, p_recv.at[0], dev(0, 0, 1)).start()
    send_m(M_STEPS[1])

    per = 128 // opm

    def outer(h, slots):
        b_line = b_row[h * n_x:(h + 1) * n_x].reshape(line * opm, n_seq)
        a_pair = jnp.concatenate([a_all[k] for k in slots], axis=1)
        both = jnp.dot(b_line, a_pair, preferred_element_type=F32)
        for t in range(len(slots)):
            o_s[t] = both[:, t * rows * opm:(t + 1) * rows * opm]
        for g in range(opm // per):
            for t in range(len(slots)):
                parts = [o_s[t, pl.ds(g * per + q, line, stride=opm), :].astype(BF16) for q in range(per)]
                for i in range(rows):
                    block = jnp.concatenate([v[:, i * opm:(i + 1) * opm] for v in parts], axis=1)
                    to = (t * rows + i) * line
                    lhs_s[to:to + line, g * 128:(g + 1) * 128] = block.astype(BF16)
        res = jnp.dot(lhs_s[:len(slots) * rows * line], w_perm[...], preferred_element_type=F32)
        return [res[t * rows * line:(t + 1) * rows * line] for t in range(len(slots))]

    def finish(h, res, row):
        for i in range(rows):
            for t in range(n_x):
                at = pl.ds((row * n_x + t) * 2 * rows + cs[h] * rows, rows)
                part = res[(i * n_x + t) * rows:(i * n_x + t + 1) * rows]
                pair_ref[i, at, :] += (part + bias_out) * den_s[i, at, :]

    for h in range(2):
        if h == 1:
            wait_in(b_row.at[pl.ds(n_x, n_x)], p_recv.at[0])
        for slots in (order_y[:1], order_y[1:]):
            if h == 0:
                for k in slots:
                    wait_in(a_all.at[k], a_recv.at[k])
            for k, res in zip(slots, outer(h, slots), strict=True):
                r_send[k, h] = res
                remote(r_send.at[k, h], r_got.at[k, h], r_ssem, r_rsem.at[k, h], dev(n_y - k, 0, 0)).start()
    send_m(len(left))
    for h in range(2):
        finish(h, outer(h, [0])[0], y)
    arrived = m_got.at[pl.ds(0, n_dev - 1)]
    wait_in(arrived, m_recv)
    keep.wait()
    for s in range(seq_own):
        msa_ref[s] = m_got[:, s].astype(F32).reshape(n_res, chans).astype(BF16)
    for h in range(2):
        for k in order_y:
            wait_in(r_got.at[k, h], r_rsem.at[k, h])
            finish(h, r_got[k, h], ys[k])

    for ref, sem in [
        (arrived, m_send), (a_all.at[pl.ds(0, n_y - 1)], a_send), (b_row.at[pl.ds(0, n_x - 1)], b_send),
        (b_row.at[pl.ds(0, n_x)], p_send), (r_send.at[pl.ds(0, n_y - 1)], r_ssem),
    ]:
        remote(ref, ref, sem, sem, dev(0, 0, 1)).wait_send()


def store(pair_v, msa_v, pair_ref, msa_ref, sem):
    copies = [pltpu.make_async_copy(pair_v, pair_ref, sem.at[0]), pltpu.make_async_copy(msa_v, msa_ref, sem.at[1])]
    for copy in copies:
        copy.start()
    for copy in copies:
        copy.wait()


def solution(mesh):
    n_y, n_dap = mesh.shape["outer"], mesh.shape["dap"]
    n_x, n_dev = n_dap // 2, n_y * n_dap
    dap_axes = ("outer", "dap")
    group_axes = ("data", "outer", "dap")

    def local_step(msa, mask, pair, gamma, beta, w_left, b_left, w_right, b_right, w_out, b_out):
        n_seq, rows, chans = msa.shape
        n_res = mask.shape[1]
        opm = w_left.shape[1]
        pair_dim = w_out.shape[1]
        seq_own = n_seq // n_dev
        line = n_x * rows
        dma = pltpu.SemaphoreType.DMA
        vmem = pl.BlockSpec(memory_space=pltpu.VMEM)
        ins = (msa, mask, pair, gamma, beta, w_left.T, b_left, w_right.T, b_right, w_out, b_out)
        got = pl.pallas_call(
            functools.partial(kernel, n_y, n_dap),
            out_shape=(
                pltpu.VMEM(pair.shape, F32),
                pltpu.VMEM((seq_own, n_dev * rows, chans), BF16),
            ),
            in_specs=[pl.BlockSpec(memory_space=pl.ANY)] * len(ins),
            out_specs=(vmem, vmem),
            scratch_shapes=[pltpu.VMEM(v.shape, v.dtype) for v in ins[:2] + ins[3:]] + [
                pltpu.VMEM((n_dev, seq_own, rows, chans), BF16),
                pltpu.VMEM((n_seq * rows, 2 * opm), F32),
                pltpu.VMEM((n_y, n_seq, rows * opm), BF16),
                pltpu.VMEM((n_dap, rows * opm, n_seq), BF16),
                pltpu.VMEM((2, line * opm, rows * opm), F32),
                pltpu.VMEM((opm * opm, pair_dim), F32),
                pltpu.VMEM((opm * opm, pair_dim), BF16),
                pltpu.VMEM((2 * rows * line, opm * opm), BF16),
                pltpu.VMEM((rows, n_res, pair_dim), F32),
                pltpu.VMEM((n_y, 2, rows * line, pair_dim), F32),
                pltpu.VMEM((n_y, 2, rows * line, pair_dim), F32),
                dma((10,)), dma((LN_CHUNKS,)), dma, dma, dma,
                dma, dma((n_y,)), dma, dma((n_x,)), dma, dma((1,)), dma, dma((n_y, 2)),
            ],
            compiler_params=pltpu.CompilerParams(collective_id=0, has_side_effects=True),
        )(*ins)
        return pl.pallas_call(
            store,
            out_shape=tuple(jax.ShapeDtypeStruct(v.shape, v.dtype) for v in got),
            in_specs=[pl.BlockSpec(memory_space=pl.ANY)] * 2,
            out_specs=(pl.BlockSpec(memory_space=pl.ANY),) * 2,
            scratch_shapes=[dma((2,))],
            compiler_params=pltpu.CompilerParams(vmem_limit_bytes=4 * 1024 * 1024),
        )(*got)

    return jax.shard_map(
        local_step, mesh=mesh,
        in_specs=(P("data", dap_axes, None), P("data", None), P(group_axes, None, None)) + (P(),) * 8,
        out_specs=(P(group_axes, None, None), P(group_axes, None, None)), check_vma=False,
    )
```
